8 devices in a mesh: dp: 8 (over z, y, x, core).
Axes of the slice: x: 2, y: 2, z: 1, core: 2. Of those that a mesh axis runs over, the one named last changes fastest.
Arguments:
- u_norm: bfloat16 [16, 2048, 1536], P(None, 'dp')
- expert_idx: int32 [16, 2048, 8], P(None, 'dp')
- expert_out: bfloat16 [16, 2048, 8, 1536], P(None, 'dp')
- d_out: bfloat16 [16, 2048, 1536], P(None, 'dp')
- w_router: bfloat16 [16, 1536, 40], replicated
Outputs:
- output 1: float32 [], replicated
- output 2: float32 [16, 1536, 40], replicated
- output 3: bfloat16 [16, 2048, 1536], P(None, 'dp')
All inputs are finite; a program needn't handle non-finite values.
Results may differ from the reference program's by a relative error of at most 0.00903813.
Values sent between devices are 32-bit elements.
A program may use at most 1 GiB of HBM per device.

```python
import jax
import jax.numpy as jnp
from jax import lax

LAYERS = 16
GROUP = 8
TOK_DEV = 256
D = 1536
EXPERTS = 40
TOP = 8

TOKENS = GROUP * TOK_DEV
AUX_COEF = 0.02
LOSS_SCALE = 1.0 * TOKENS
DY_SCALE = 0.015 * (TOP / (EXPERTS * TOKENS * D)) ** 0.5


def draw_slots(slot_key):
    expert_ids = jnp.arange(EXPERTS)
    tok_pos = jnp.arange(TOKENS)
    tok_owner = tok_pos // TOK_DEV
    favored = (expert_ids[None, :] == (tok_owner % EXPERTS)[:, None]).astype(jnp.int32)
    weights = 1 + expert_ids[None, :] % 3 + 12 * favored
    tickets = jax.random.randint(slot_key, (LAYERS, TOKENS, EXPERTS), 0, 4096)
    int_score = weights[None] * tickets * EXPERTS + expert_ids
    drawn_ids = lax.top_k(int_score, TOP)[1]
    forced = (tok_pos[:, None] + jnp.arange(TOP)[None, :]) % EXPERTS
    chosen_ids = jnp.where((tok_pos < EXPERTS)[None, :, None], forced[None], drawn_ids)
    return chosen_ids.astype(jnp.int32)


def setup_inputs(seed: int = 0) -> dict:
    base_key = jax.random.key(seed)
    key_list = jax.random.split(base_key, 7)
    global_mean = 0.5 * jax.random.normal(key_list[0], (LAYERS, 1, D), jnp.float32)
    device_mean = 0.5 * jax.random.normal(key_list[1], (LAYERS, GROUP, 1, D), jnp.float32)
    noise_vals = jax.random.normal(key_list[2], (LAYERS, GROUP, TOK_DEV, D), jnp.float32)
    u_vals = (noise_vals + device_mean).reshape(LAYERS, TOKENS, D) + global_mean
    expert_out = jax.random.normal(key_list[4], (LAYERS, TOKENS, TOP, D), jnp.float32)
    d_out = DY_SCALE * jax.random.normal(key_list[5], (LAYERS, TOKENS, D), jnp.float32)
    w_router = jax.random.normal(key_list[6], (LAYERS, D, EXPERTS), jnp.float32) * D ** -0.5
    return {
        'u_norm': u_vals.astype(jnp.bfloat16),
        'expert_idx': draw_slots(key_list[3]),
        'expert_out': expert_out.astype(jnp.bfloat16),
        'd_out': d_out.astype(jnp.bfloat16),
        'w_router': w_router.astype(jnp.bfloat16),
    }


def reference(u_norm, expert_idx, expert_out, d_out, w_router):
    def one_layer(layer_in):
        u_layer, idx_layer, out_layer, dy_layer, w_layer = layer_in
        logits = jnp.dot(u_layer, w_layer, preferred_element_type=jnp.float32)
        slot_dots = jnp.einsum('tkd,td->tk', out_layer.astype(jnp.float32), dy_layer.astype(jnp.float32))
        one_hot = jax.nn.one_hot(idx_layer, EXPERTS, dtype=jnp.float32)
        exp_frac = jnp.sum(one_hot, axis=(0, 1)) / (TOP * TOKENS)

        def loss_of(logit_in):
            prob_vals = jax.nn.softmax(logit_in, axis=-1)
            gate_vals = jax.nn.softmax(jnp.take_along_axis(logit_in, idx_layer, axis=-1), axis=-1)
            main_part = jnp.sum(gate_vals * slot_dots)
            aux_part = EXPERTS * jnp.sum(exp_frac * jnp.mean(prob_vals, axis=0))
            return main_part + AUX_COEF * aux_part

        layer_loss, pull_back = jax.vjp(loss_of, logits)
        d_logits = pull_back(jnp.ones_like(layer_loss) * LOSS_SCALE)[0]
        d_log16 = d_logits.astype(jnp.bfloat16)
        grad_w = jnp.dot(u_layer.T, d_log16, preferred_element_type=jnp.float32)
        grad_u = jnp.dot(d_log16, w_layer.T, preferred_element_type=jnp.float32).astype(jnp.bfloat16)
        return layer_loss, grad_w, grad_u

    layer_losses, d_router, d_norm = lax.map(one_layer, (u_norm, expert_idx, expert_out, d_out, w_router))
    return (jnp.sum(layer_losses), d_router, d_norm)
```

```python
import functools

import jax
import jax.numpy as jnp
from jax import lax
from jax.experimental import pallas as pl
from jax.experimental.pallas import tpu as pltpu
from jax.sharding import PartitionSpec as P

AUX_COEF = 0.02
MESH = pl.DeviceIdType.MESH
RING_E = 6
RING_U = 4
RING_D = 3
LANES = 128


def stream_kernel(tok_all, idx_hbm, w_hbm, u_hbm, d_hbm, e_hbm,
                  gt_hbm, r_hbm, loss_hbm,
                  idx_v, w_v, u_v, d_v, e_v, sd_a, sd_b, cnt, rst, frac, gt_v,
                  part, rd1, rrs, rex, red, lacc, lvals,
                  in_sem, e_sem, u_sem, d_sem,
                  st_s, st_r, d1_s, d1_r, rs_s, rs_r, ex_s, ex_r, ag_s, ag_r, d2_s, d2_r,
                  ls_s, ls_r, out_sem, gt_sem):
    layers, top_k, tok = idx_v.shape
    num_exp = w_v.shape[1]
    half = tok // 2
    rows = half * top_k
    tiles = part.shape[1]
    n_dev = rst.shape[0]
    scale = float(tok_all)
    coef = AUX_COEF * num_exp

    me = lax.axis_index('dp')
    core = me % 2
    x = (me // 2) % 2
    y = me // 4
    mate = me + 1 - 2 * core
    x_peer = me + 2 - 4 * x
    y_peer = me + 4 - 8 * y
    big1 = x_peer * (1 - core) + y_peer * core
    big2 = y_peer * (1 - core) + x_peer * core
    hb = x * (1 - core) + y * core
    hs = y * (1 - core) + x * core
    base = 6 * core
    big_keep = base + 2 * hb
    big_send = base + 2 * (1 - hb)
    small_keep = base + 4 + hs
    small_send = base + 4 + (1 - hs)

    def remote(src, dst, send, recv, dev):
        return pltpu.make_async_remote_copy(src_ref=src, dst_ref=dst, send_sem=send, recv_sem=recv,
                                            device_id=(dev,), device_id_type=MESH)

    def e_copy(c):
        return pltpu.make_async_copy(e_hbm.at[c // 2, pl.ds((c % 2) * rows, rows)], e_v.at[c % RING_E], e_sem.at[c % RING_E])

    def u_copy(l):
        return pltpu.make_async_copy(u_hbm.at[l], u_v.at[l % RING_U], u_sem.at[l % RING_U])

    def d_copy(l):
        return pltpu.make_async_copy(d_hbm.at[l], d_v.at[l % RING_D], d_sem.at[l % RING_D])

    idx_copy = pltpu.make_async_copy(idx_hbm, idx_v, in_sem.at[0])
    w_copy = pltpu.make_async_copy(w_hbm, w_v, in_sem.at[1])
    idx_copy.start()
    d_copy(0).start()
    e_copy(0).start()
    e_copy(1).start()
    w_copy.start()
    u_copy(0).start()
    for l in range(1, 3):
        d_copy(l).start()
        e_copy(2 * l).start()
        e_copy(2 * l + 1).start()
        u_copy(l).start()
    u_copy(3).start()

    barrier = pltpu.get_barrier_semaphore()
    for r in range(1, n_dev):
        pl.semaphore_signal(barrier, inc=1, device_id=((me + r) % n_dev,), device_id_type=MESH)

    exp_iota = lax.broadcasted_iota(jnp.int32, (num_exp, tok), 0)
    lane_e = lax.broadcasted_iota(jnp.int32, (num_exp, LANES), 1)
    lane_8 = lax.broadcasted_iota(jnp.int32, (top_k, LANES), 1)
    idx_copy.wait()

    def count_layer(l, acc):
        ids = idx_v[l]
        hit = jnp.zeros((num_exp, tok), jnp.float32)
        for k in range(top_k):
            hit = hit + jnp.where(ids[k:k + 1, :] == exp_iota, 1.0, 0.0)
        col = jnp.sum(hit, axis=1, keepdims=True)
        return jnp.where(lane_e == l, col, acc)

    cnt[...] = lax.fori_loop(0, layers, count_layer, jnp.zeros((num_exp, LANES), jnp.float32))
    lacc[...] = jnp.zeros_like(lacc)
    w_copy.wait()
    pl.semaphore_wait(barrier, n_dev - 1)

    def stat_copy(r):
        return remote(cnt, rst.at[r], st_s.at[r], st_r.at[r], (me + r) % n_dev)

    for r in range(1, n_dev):
        stat_copy(r).start()

    def d1_copy(l):
        return remote(part.at[l, pl.ds(6 * (1 - core), 6)], rd1.at[l], d1_s.at[l], d1_r.at[l], mate)

    def rs_copies(l):
        return (remote(part.at[l, pl.ds(big_send, 2)], rrs.at[l, pl.ds(0, 2)], rs_s.at[0, l], rs_r.at[0, l], big1),
                remote(part.at[l, pl.ds(small_send, 1)], rrs.at[l, pl.ds(2, 1)], rs_s.at[1, l], rs_r.at[1, l], big2))

    def ex_copies(l):
        return (remote(part.at[l, pl.ds(big_keep, 2)], rex.at[l, pl.ds(0, 2)], ex_s.at[0, l], ex_r.at[0, l], big2),
                remote(part.at[l, pl.ds(small_keep, 1)], rex.at[l, pl.ds(2, 1)], ex_s.at[1, l], ex_r.at[1, l], big1))

    def ag_copies(l):
        return (remote(red.at[l, pl.ds(big_keep, 2)], red.at[l, pl.ds(big_keep, 2)], ag_s.at[0, l], ag_r.at[0, l], big1),
                remote(red.at[l, pl.ds(small_keep, 1)], red.at[l, pl.ds(small_keep, 1)], ag_s.at[1, l], ag_r.at[1, l], big2))

    def d2_copy(l):
        return remote(red.at[l, pl.ds(base, 6)], red.at[l, pl.ds(base, 6)], d2_s.at[l], d2_r.at[l], mate)

    def out_copy(l):
        return pltpu.make_async_copy(red.at[l], r_hbm.at[l], out_sem.at[l])

    def when_layer(l, fn):
        pl.when(jnp.logical_and(l >= 0, l < layers))(lambda: fn(l))

    def act_d1(l):
        d1_copy(l).start()

    def act_rs(l):
        d1_copy(l).wait()
        for i in range(6):
            part[l, base + i] = part[l, base + i] + rd1[l, i]
        for c in rs_copies(l):
            c.start()

    def act_ex(l):
        for c in rs_copies(l):
            c.wait()
        for i in range(2):
            part[l, big_keep + i] = part[l, big_keep + i] + rrs[l, i]
        part[l, small_keep] = part[l, small_keep] + rrs[l, 2]
        for c in ex_copies(l):
            c.start()

    def act_ag(l):
        for c in ex_copies(l):
            c.wait()
        for i in range(2):
            red[l, big_keep + i] = part[l, big_keep + i] + rex[l, i]
        red[l, small_keep] = part[l, small_keep] + rex[l, 2]
        for c in ag_copies(l):
            c.start()

    def act_d2(l):
        for c in ag_copies(l):
            c.wait()
        d2_copy(l).start()

    def act_out(l):
        d2_copy(l).wait()
        out_copy(l).start()

    def slots(s, h, sd):
        c = 2 * s + h
        dref = d_v[s % RING_D, pl.ds(h * half, half), :]
        prod = lax.dot_general(e_v[c % RING_E], dref, (((1,), (1,)), ((), ())), preferred_element_type=jnp.float32)
        accs = [jnp.zeros((top_k, LANES), jnp.float32) for _ in range(4)]
        for t in range(half):
            accs[t % 4] = jnp.where(lane_8 == t, prod[t * top_k:(t + 1) * top_k, :], accs[t % 4])
        sd[...] = (accs[0] + accs[1]) + (accs[2] + accs[3])

    def finish(l):
        u = u_v[l % RING_U]
        w = w_v[l]
        logits = lax.dot_general(w, u, (((1,), (1,)), ((), ())), preferred_element_type=jnp.float32)
        ids = idx_v[l]
        dots = jnp.concatenate([sd_a[...], sd_b[...]], axis=1) * scale
        sel = ids[0:1, :] == exp_iota
        dd = jnp.where(sel, dots[0:1, :], 0.0)
        for k in range(1, top_k):
            hit = ids[k:k + 1, :] == exp_iota
            dd = jnp.where(hit, dots[k:k + 1, :], dd)
            sel = jnp.logical_or(sel, hit)
        top = jnp.max(logits, axis=0, keepdims=True)
        ev = jnp.exp(logits - top)
        prob = ev / jnp.sum(ev, axis=0, keepdims=True)
        low = jnp.where(sel, logits, -jnp.inf)
        top_sel = jnp.max(low, axis=0, keepdims=True)
        es = jnp.where(sel, jnp.exp(jnp.minimum(logits - top_sel, 0.0)), 0.0)
        gate = es / jnp.sum(es, axis=0, keepdims=True)
        inner = jnp.sum(gate * dd, axis=0, keepdims=True)
        pull = jnp.sum(jnp.where(lane_e == l, frac[...], 0.0), axis=1, keepdims=True)
        pin = jnp.sum(prob * pull, axis=0, keepdims=True)
        grad = gate * (dd - inner) + prob * (pull - pin)
        g16 = grad.astype(jnp.bfloat16)
        gt_v[l] = g16
        lacc[...] = lacc[...] + (inner + pin)
        pg = jnp.dot(g16, u, preferred_element_type=jnp.float32)
        for t in range(tiles):
            part[l, t] = pg[:, t * LANES:(t + 1) * LANES]

    def step(s, carry):
        when_layer(s - 2, act_rs)
        when_layer(s - 3, act_ex)
        when_layer(s - 6, act_out)

        @pl.when(s == 1)
        def _():
            total = cnt[...]
            for r in range(1, n_dev):
                stat_copy(r).wait()
                total = total + rst[r]
            frac[...] = total * (coef / (top_k * tok_all))

        @pl.when(s < layers)
        def _():
            d_copy(s).wait()
            e_copy(2 * s).wait()

        @pl.when(jnp.logical_and(s >= 1, s <= layers))
        def _():
            u_copy(s - 1).wait()

        @pl.when(s == 0)
        def _():
            slots(s, 0, sd_a)

        @pl.when(jnp.logical_and(s >= 1, s < layers))
        def _():
            finish(s - 1)
            slots(s, 0, sd_a)

        @pl.when(s == layers)
        def _():
            finish(s - 1)

        @pl.when(2 * s + RING_E < 2 * layers)
        def _():
            e_copy(2 * s + RING_E).start()

        @pl.when(jnp.logical_and(s >= 1, s - 1 + RING_U < layers))
        def _():
            u_copy(s - 1 + RING_U).start()

        when_layer(s - 5, act_d2)
        when_layer(s - 4, act_ag)
        when_layer(s - 1, act_d1)

        @pl.when(s < layers)
        def _():
            e_copy(2 * s + 1).wait()
            slots(s, 1, sd_b)

        @pl.when(2 * s + 1 + RING_E < 2 * layers)
        def _():
            e_copy(2 * s + 1 + RING_E).start()

        @pl.when(s + RING_D < layers)
        def _():
            d_copy(s + RING_D).start()

        @pl.when(s == layers)
        def _():
            gt_copy.start()
            lvals[me] = jnp.broadcast_to(jnp.sum(lacc[...], axis=1, keepdims=True) * (1.0 / scale), (8, LANES))
            for r in range(1, n_dev):
                loss_copy(r).start()

        return carry

    gt_copy = pltpu.make_async_copy(gt_v, gt_hbm, gt_sem.at[0])

    def loss_copy(r):
        return remote(lvals.at[me], lvals.at[me], ls_s.at[r], ls_r.at[r], (me + r) % n_dev)

    lax.fori_loop(0, layers + 6, step, 0)

    for r in range(1, n_dev):
        loss_copy(r).wait()
    total = lvals[0]
    for r in range(1, n_dev):
        total = total + lvals[r]
    lacc[...] = jnp.concatenate([total[0:1, :], total[0:1, :]], axis=1)
    loss_out = pltpu.make_async_copy(lacc, loss_hbm, gt_sem.at[1])
    loss_out.start()
    gt_copy.wait()
    for l in range(layers):
        out_copy(l).wait()
    loss_out.wait()


def finish_kernel(gt_ref, w_ref, r_ref, loss_in, dn_ref, dr_ref, loss_ref):
    for i in range(gt_ref.shape[0]):
        dn_ref[i] = lax.dot_general(gt_ref[i], w_ref[i], (((0,), (0,)), ((), ())),
                                    preferred_element_type=jnp.float32).astype(jnp.bfloat16)
        for t in range(r_ref.shape[1]):
            dr_ref[i, :, t * LANES:(t + 1) * LANES] = r_ref[i, t]
    loss_ref[0] = loss_in[0, 0]


def solution(mesh):
    group_size = mesh.shape['dp']

    def local_step(u_norm, expert_idx, expert_out, d_out, w_router):
        layers, tok, dim = u_norm.shape
        top_k = expert_idx.shape[2]
        num_exp = w_router.shape[2]
        tiles = dim // LANES
        idx_t = jnp.transpose(expert_idx, (0, 2, 1))
        w_t = jnp.transpose(w_router, (0, 2, 1))
        e_flat = expert_out.reshape(layers, tok * top_k, dim)
        any_spec = pl.BlockSpec(memory_space=pl.ANY)
        dma = pltpu.SemaphoreType.DMA
        f32, b16 = jnp.float32, jnp.bfloat16
        gt, red, loss = pl.pallas_call(
            functools.partial(stream_kernel, tok * group_size),
            out_shape=(jax.ShapeDtypeStruct((layers, num_exp, tok), b16),
                       jax.ShapeDtypeStruct((layers, tiles, num_exp, LANES), f32),
                       jax.ShapeDtypeStruct((1, tok), f32)),
            in_specs=[any_spec] * 5,
            out_specs=(any_spec,) * 3,
            scratch_shapes=[
                pltpu.VMEM((layers, top_k, tok), jnp.int32),
                pltpu.VMEM((layers, num_exp, dim), b16),
                pltpu.VMEM((RING_U, tok, dim), b16),
                pltpu.VMEM((RING_D, tok, dim), b16),
                pltpu.VMEM((RING_E, tok * top_k // 2, dim), b16),
                pltpu.VMEM((top_k, LANES), f32),
                pltpu.VMEM((top_k, LANES), f32),
                pltpu.VMEM((num_exp, LANES), f32),
                pltpu.VMEM((group_size, num_exp, LANES), f32),
                pltpu.VMEM((num_exp, LANES), f32),
                pltpu.VMEM((layers, num_exp, tok), b16),
                pltpu.VMEM((layers, tiles, num_exp, LANES), f32),
                pltpu.VMEM((layers, tiles // 2, num_exp, LANES), f32),
                pltpu.VMEM((layers, 3, num_exp, LANES), f32),
                pltpu.VMEM((layers, 3, num_exp, LANES), f32),
                pltpu.VMEM((layers, tiles, num_exp, LANES), f32),
                pltpu.VMEM((1, tok), f32),
                pltpu.VMEM((group_size, 8, LANES), f32),
                dma((2,)), dma((RING_E,)), dma((RING_U,)), dma((RING_D,)),
                dma((group_size,)), dma((group_size,)),
                dma((layers,)), dma((layers,)),
                dma((2, layers)), dma((2, layers)),
                dma((2, layers)), dma((2, layers)),
                dma((2, layers)), dma((2, layers)),
                dma((layers,)), dma((layers,)),
                dma((group_size,)), dma((group_size,)),
                dma((layers,)), dma((2,)),
            ],
            compiler_params=pltpu.CompilerParams(collective_id=0, has_side_effects=True,
                                                 vmem_limit_bytes=56 * 1024 * 1024),
            name='router_stream',
        )(idx_t, w_t, u_norm, d_out, e_flat)
        blk = 2
        d_norm, dr_t, loss1 = pl.pallas_call(
            finish_kernel,
            grid=(layers // blk,),
            out_shape=(jax.ShapeDtypeStruct((layers, tok, dim), b16),
                       jax.ShapeDtypeStruct((layers, num_exp, dim), f32),
                       jax.ShapeDtypeStruct((1,), f32)),
            in_specs=[pl.BlockSpec((blk, num_exp, tok), lambda i: (i, 0, 0)),
                      pl.BlockSpec((blk, num_exp, dim), lambda i: (i, 0, 0)),
                      pl.BlockSpec((blk, tiles, num_exp, LANES), lambda i: (i, 0, 0, 0)),
                      pl.BlockSpec((1, tok), lambda i: (0, 0), memory_space=pltpu.SMEM)],
            out_specs=(pl.BlockSpec((blk, tok, dim), lambda i: (i, 0, 0)),
                       pl.BlockSpec((blk, num_exp, dim), lambda i: (i, 0, 0)),
                       pl.BlockSpec((1,), lambda i: (0,), memory_space=pltpu.SMEM)),
            name='router_outputs',
        )(gt, w_t, red, loss)
        return loss1.reshape(()), jnp.transpose(dr_t, (0, 2, 1)), d_norm

    tok_spec = P(None, 'dp', None)
    return jax.shard_map(local_step, mesh=mesh, in_specs=(tok_spec, tok_spec, P(None, 'dp', None, None), tok_spec, P()), out_specs=(P(), P(), tok_spec), check_vma=False)
```

```python
import functools

import jax
import jax.numpy as jnp
from jax import lax
from jax.experimental import pallas as pl
from jax.experimental.pallas import tpu as pltpu
from jax.sharding import PartitionSpec as P

AUX_COEF = 0.02
MESH = pl.DeviceIdType.MESH
RING_E = 6
RING_U = 4
RING_D = 3
RING_P = 8
LANES = 128
OFFS = (3, 5, 9, 13, 17, 19)


def stream_kernel(tok_all, idx_hbm, w_hbm, u_hbm, d_hbm, e_hbm,
                  dn, red, loss_out,
                  idx_v, w_v, u_v, d_v, e_v, sd_a, sd_b, df_a, df_b, cnt, rst, frac, gt_v,
                  part, rd1, rrs, rex, lacc, lvals,
                  in_sem, e_sem, u_sem, d_sem,
                  st_s, st_r, d1_s, d1_r, rs_s, rs_r, ex_s, ex_r, ag_s, ag_r, d2_s, d2_r,
                  ls_s, ls_r):
    layers, top_k, tok = idx_v.shape
    num_exp = w_v.shape[1]
    half = tok // 2
    rows = half * top_k
    tiles = part.shape[1]
    n_dev = rst.shape[0]
    scale = float(tok_all)
    coef = AUX_COEF * num_exp

    me = lax.axis_index('dp')
    core = me % 2
    x = (me // 2) % 2
    y = me // 4
    mate = me + 1 - 2 * core
    x_peer = me + 2 - 4 * x
    y_peer = me + 4 - 8 * y
    big1 = x_peer * (1 - core) + y_peer * core
    big2 = y_peer * (1 - core) + x_peer * core
    hb = x * (1 - core) + y * core
    hs = y * (1 - core) + x * core
    base = 6 * core
    big_keep = base + 2 * hb
    big_send = base + 2 * (1 - hb)
    small_keep = base + 4 + hs
    small_send = base + 4 + (1 - hs)

    def remote(src, dst, send, recv, dev):
        return pltpu.make_async_remote_copy(src_ref=src, dst_ref=dst, send_sem=send, recv_sem=recv,
                                            device_id=(dev,), device_id_type=MESH)

    def e_copy(c):
        return pltpu.make_async_copy(e_hbm.at[c // 2, pl.ds((c % 2) * rows, rows)], e_v.at[c % RING_E], e_sem.at[c % RING_E])

    def u_copy(l):
        return pltpu.make_async_copy(u_hbm.at[l], u_v.at[l % RING_U], u_sem.at[l % RING_U])

    def d_copy(l):
        return pltpu.make_async_copy(d_hbm.at[l], d_v.at[l % RING_D], d_sem.at[l % RING_D])

    idx_copy = pltpu.make_async_copy(idx_hbm, idx_v, in_sem.at[0])
    w_copy = pltpu.make_async_copy(w_hbm, w_v, in_sem.at[1])
    idx_copy.start()
    d_copy(0).start()
    e_copy(0).start()
    e_copy(1).start()
    w_copy.start()
    u_copy(0).start()
    for l in range(1, 3):
        d_copy(l).start()
        e_copy(2 * l).start()
        e_copy(2 * l + 1).start()
        u_copy(l).start()
    u_copy(3).start()

    barrier = pltpu.get_barrier_semaphore()
    for r in range(1, n_dev):
        pl.semaphore_signal(barrier, inc=1, device_id=((me + r) % n_dev,), device_id_type=MESH)

    exp_iota = lax.broadcasted_iota(jnp.int32, (num_exp, tok), 0)
    lane_e = lax.broadcasted_iota(jnp.int32, (num_exp, LANES), 1)
    lane_8 = lax.broadcasted_iota(jnp.int32, (top_k, LANES), 1)
    idx_copy.wait()

    def count_layer(l, acc):
        ids = idx_v[l]
        hit = jnp.zeros((num_exp, tok), jnp.float32)
        for k in range(top_k):
            hit = hit + jnp.where(ids[k:k + 1, :] == exp_iota, 1.0, 0.0)
        col = jnp.sum(hit, axis=1, keepdims=True)
        return jnp.where(lane_e == l, col, acc)

    cnt[...] = lax.fori_loop(0, layers, count_layer, jnp.zeros((num_exp, LANES), jnp.float32))
    lacc[...] = jnp.zeros_like(lacc)
    pl.semaphore_wait(barrier, n_dev - 1)

    def stat_copy(r):
        return remote(cnt, rst.at[r], st_s.at[r], st_r.at[r], (me + r) % n_dev)

    for r in range(1, n_dev):
        stat_copy(r).start()

    def cols(l, tile, n):
        return red.at[l, :, pl.ds(pl.multiple_of(tile * LANES, LANES), n * LANES)]

    def d1_copy(l):
        return remote(part.at[l % RING_P, pl.ds(6 * (1 - core), 6)], rd1.at[l], d1_s.at[l], d1_r.at[l], mate)

    def rs_copies(l):
        return (remote(part.at[l % RING_P, pl.ds(big_send, 2)], rrs.at[l, pl.ds(0, 2)], rs_s.at[0, l], rs_r.at[0, l], big1),
                remote(part.at[l % RING_P, pl.ds(small_send, 1)], rrs.at[l, pl.ds(2, 1)], rs_s.at[1, l], rs_r.at[1, l], big2))

    def ex_copies(l):
        return (remote(part.at[l % RING_P, pl.ds(big_keep, 2)], rex.at[l, pl.ds(0, 2)], ex_s.at[0, l], ex_r.at[0, l], big2),
                remote(part.at[l % RING_P, pl.ds(small_keep, 1)], rex.at[l, pl.ds(2, 1)], ex_s.at[1, l], ex_r.at[1, l], big1))

    def ag_copies(l):
        big, small = cols(l, big_keep, 2), cols(l, small_keep, 1)
        return (remote(big, big, ag_s.at[0, l], ag_r.at[0, l], big1),
                remote(small, small, ag_s.at[1, l], ag_r.at[1, l], big2))

    def d2_copy(l):
        return remote(cols(l, base, 6), cols(l, base, 6), d2_s.at[l], d2_r.at[l], mate)

    def when_layer(l, fn):
        pl.when(jnp.logical_and(l >= 0, l < layers))(lambda: fn(l))

    def act_d1(l):
        d1_copy(l).start()

    def act_rs(l):
        d1_copy(l).wait()
        for i in range(6):
            part[l % RING_P, base + i] = part[l % RING_P, base + i] + rd1[l, i]
        for c in rs_copies(l):
            c.start()

    def act_ex(l):
        for c in rs_copies(l):
            c.wait()
        for i in range(2):
            part[l % RING_P, big_keep + i] = part[l % RING_P, big_keep + i] + rrs[l, i]
        part[l % RING_P, small_keep] = part[l % RING_P, small_keep] + rrs[l, 2]
        for c in ex_copies(l):
            c.start()

    def act_ag(l):
        for c in ex_copies(l):
            c.wait()
        for i in range(2):
            cols(l, big_keep + i, 1)[...] = part[l % RING_P, big_keep + i] + rex[l, i]
        cols(l, small_keep, 1)[...] = part[l % RING_P, small_keep] + rex[l, 2]
        for c in ag_copies(l):
            c.start()

    def act_d2(l):
        for c in ag_copies(l):
            c.wait()
        d2_copy(l).start()

    def act_out(l):
        d2_copy(l).wait()

    def slots(s, h, sd, df):
        c = 2 * s + h
        df[...] = d_v[s % RING_D, pl.ds(h * half, half), :].astype(jnp.float32)
        acc = jnp.zeros((top_k, LANES), jnp.float32)
        nm = 48
        dref = d_v[s % RING_D, pl.ds(h * half + half - nm, nm), :]
        mm = lax.dot_general(e_v[c % RING_E, (half - nm) * top_k:, :], dref, (((1,), (1,)), ((), ())), preferred_element_type=jnp.float32)
        acc2 = jnp.zeros((top_k, nm), jnp.float32)
        lane_m = lax.broadcasted_iota(jnp.int32, (top_k, nm), 1)
        for t in range(nm):
            acc2 = jnp.where(lane_m == t, mm[t * top_k:(t + 1) * top_k, :], acc2)
        for p in range((half - nm) // 2):
            ev = e_v[c % RING_E, 2 * top_k * p:2 * top_k * (p + 1), :].astype(jnp.float32)
            for i in range(2):
                t = 2 * p + i
                prod = ev[i * top_k:(i + 1) * top_k, :] * df[pl.ds(t, top_k, stride=0), :]
                lanes = prod[:, 0:LANES]
                for j in range(1, tiles):
                    lanes = lanes + prod[:, j * LANES:(j + 1) * LANES]
                acc = jnp.where(lane_8 == t, jnp.sum(lanes, axis=1, keepdims=True), acc)
        sd[...] = acc
        sd[:, half - nm:] = acc2

    def read_sd():
        return sd_a[...], sd_b[...]

    def finish(l, sd):
        u = u_v[l % RING_U]
        w = w_v[l]
        logits = lax.dot_general(w, u, (((1,), (1,)), ((), ())), preferred_element_type=jnp.float32)
        ids = idx_v[l]
        dots = jnp.concatenate(sd, axis=1) * scale
        sel = ids[0:1, :] == exp_iota
        dd = jnp.where(sel, dots[0:1, :], 0.0)
        for k in range(1, top_k):
            hit = ids[k:k + 1, :] == exp_iota
            dd = jnp.where(hit, dots[k:k + 1, :], dd)
            sel = jnp.logical_or(sel, hit)
        top = jnp.max(logits, axis=0, keepdims=True)
        ev = jnp.exp(logits - top)
        prob = ev / jnp.sum(ev, axis=0, keepdims=True)
        low = jnp.where(sel, logits, -jnp.inf)
        top_sel = jnp.max(low, axis=0, keepdims=True)
        es = jnp.where(sel, jnp.exp(jnp.minimum(logits - top_sel, 0.0)), 0.0)
        gate = es / jnp.sum(es, axis=0, keepdims=True)
        inner = jnp.sum(gate * dd, axis=0, keepdims=True)
        pull = jnp.sum(jnp.where(lane_e == l, frac[...], 0.0), axis=1, keepdims=True)
        pin = jnp.sum(prob * pull, axis=0, keepdims=True)
        grad = gate * (dd - inner) + prob * (pull - pin)
        g16 = grad.astype(jnp.bfloat16)
        gt_v[l] = g16
        lacc[...] = lacc[...] + (inner + pin)
        pg = jnp.dot(g16, u, preferred_element_type=jnp.float32)
        for t in range(tiles):
            part[l % RING_P, t] = pg[:, t * LANES:(t + 1) * LANES]

    def comm(s, h):
        for off, fn in SCHEDULE:
            if (off - h) % 2 == 0:
                when_layer(s - (off - h) // 2, fn)

    def step(s, carry):
        comm(s, 0)

        @pl.when(s == 1)
        def _():
            total = cnt[...]
            for r in range(1, n_dev):
                stat_copy(r).wait()
                total = total + rst[r]
            frac[...] = total * (coef / (top_k * tok_all))
            w_copy.wait()

        @pl.when(s < layers)
        def _():
            d_copy(s).wait()
            e_copy(2 * s).wait()

        @pl.when(jnp.logical_and(s >= 1, s <= layers))
        def _():
            u_copy(s - 1).wait()

        @pl.when(s == 0)
        def _():
            slots(s, 0, sd_a, df_a)

        @pl.when(jnp.logical_and(s >= 1, s < layers))
        def _():
            sd = read_sd()
            slots(s, 0, sd_a, df_a)
            finish(s - 1, sd)

        @pl.when(s == layers)
        def _():
            finish(s - 1, read_sd())

        @pl.when(2 * s + RING_E < 2 * layers)
        def _():
            e_copy(2 * s + RING_E).start()

        @pl.when(jnp.logical_and(s >= 1, s - 1 + RING_U < layers))
        def _():
            u_copy(s - 1 + RING_U).start()

        @pl.when(s > layers)
        def _():
            for i in range(2):
                l = jnp.minimum(2 * (s - layers - 1) + i, layers - 1)
                dn[l] = lax.dot_general(gt_v[l], w_v[l], (((0,), (0,)), ((), ())),
                                        preferred_element_type=jnp.float32).astype(jnp.bfloat16)

        comm(s, 1)

        @pl.when(s < layers)
        def _():
            e_copy(2 * s + 1).wait()
            slots(s, 1, sd_b, df_b)

        @pl.when(2 * s + 1 + RING_E < 2 * layers)
        def _():
            e_copy(2 * s + 1 + RING_E).start()

        @pl.when(s + RING_D < layers)
        def _():
            d_copy(s + RING_D).start()

        @pl.when(s == layers)
        def _():
            lvals[me] = jnp.broadcast_to(jnp.sum(lacc[...], axis=1, keepdims=True) * (1.0 / scale), (8, LANES))
            for r in range(1, n_dev):
                loss_copy(r).start()

        return carry

    SCHEDULE = ((OFFS[0], act_d1), (OFFS[1], act_rs), (OFFS[2], act_ex), (OFFS[3], act_ag), (OFFS[4], act_d2), (OFFS[5], act_out))

    def loss_copy(r):
        return remote(lvals.at[me], lvals.at[me], ls_s.at[r], ls_r.at[r], (me + r) % n_dev)

    lax.fori_loop(0, layers + OFFS[5] // 2, step, 0)

    for r in range(1, n_dev):
        loss_copy(r).wait()
    total = lvals[0]
    for r in range(1, n_dev):
        total = total + lvals[r]
    loss_out[0] = total[0, 0]


def store_kernel(dn_v, red_v, loss_in, dn_hbm, red_hbm, loss_ref, sem):
    loss_ref[0] = loss_in[0]
    copies = []
    for l in range(dn_v.shape[0]):
        copies.append(pltpu.make_async_copy(dn_v.at[l], dn_hbm.at[l], sem.at[0, l]))
        copies.append(pltpu.make_async_copy(red_v.at[l], red_hbm.at[l], sem.at[1, l]))
    for c in copies:
        c.start()
    for c in copies:
        c.wait()


def solution(mesh):
    group_size = mesh.shape['dp']

    def local_step(u_norm, expert_idx, expert_out, d_out, w_router):
        layers, tok, dim = u_norm.shape
        top_k = expert_idx.shape[2]
        num_exp = w_router.shape[2]
        tiles = dim // LANES
        idx_t = jnp.transpose(expert_idx, (0, 2, 1))
        w_t = jnp.transpose(w_router, (0, 2, 1))
        e_flat = expert_out.reshape(layers, tok * top_k, dim)
        any_spec = pl.BlockSpec(memory_space=pl.ANY)
        dma = pltpu.SemaphoreType.DMA
        f32, b16 = jnp.float32, jnp.bfloat16
        d_norm, red, loss = pl.pallas_call(
            functools.partial(stream_kernel, tok * group_size),
            out_shape=(pltpu.VMEM((layers, tok, dim), b16),
                       pltpu.VMEM((layers, num_exp, dim), f32),
                       jax.ShapeDtypeStruct((1,), f32)),
            in_specs=[any_spec] * 5,
            out_specs=(pl.BlockSpec(memory_space=pltpu.VMEM), pl.BlockSpec(memory_space=pltpu.VMEM),
                       pl.BlockSpec(memory_space=pltpu.SMEM)),
            scratch_shapes=[
                pltpu.VMEM((layers, top_k, tok), jnp.int32),
                pltpu.VMEM((layers, num_exp, dim), b16),
                pltpu.VMEM((RING_U, tok, dim), b16),
                pltpu.VMEM((RING_D, tok, dim), b16),
                pltpu.VMEM((RING_E, tok * top_k // 2, dim), b16),
                pltpu.VMEM((top_k, LANES), f32),
                pltpu.VMEM((top_k, LANES), f32),
                pltpu.VMEM((tok // 2, dim), f32),
                pltpu.VMEM((tok // 2, dim), f32),
                pltpu.VMEM((num_exp, LANES), f32),
                pltpu.VMEM((group_size, num_exp, LANES), f32),
                pltpu.VMEM((num_exp, LANES), f32),
                pltpu.VMEM((layers, num_exp, tok), b16),
                pltpu.VMEM((RING_P, tiles, num_exp, LANES), f32),
                pltpu.VMEM((layers, tiles // 2, num_exp, LANES), f32),
                pltpu.VMEM((layers, 3, num_exp, LANES), f32),
                pltpu.VMEM((layers, 3, num_exp, LANES), f32),
                pltpu.VMEM((1, tok), f32),
                pltpu.VMEM((group_size, 8, LANES), f32),
                dma((2,)), dma((RING_E,)), dma((RING_U,)), dma((RING_D,)),
                dma((group_size,)), dma((group_size,)),
                dma((layers,)), dma((layers,)),
                dma((2, layers)), dma((2, layers)),
                dma((2, layers)), dma((2, layers)),
                dma((2, layers)), dma((2, layers)),
                dma((layers,)), dma((layers,)),
                dma((group_size,)), dma((group_size,)),
            ],
            compiler_params=pltpu.CompilerParams(collective_id=0, has_side_effects=True,
                                                 vmem_limit_bytes=46 * 1024 * 1024),
            name='router_stream',
        )(idx_t, w_t, u_norm, d_out, e_flat)
        d_norm, red, loss = pl.pallas_call(
            store_kernel,
            out_shape=(jax.ShapeDtypeStruct(d_norm.shape, d_norm.dtype), jax.ShapeDtypeStruct(red.shape, red.dtype),
                       jax.ShapeDtypeStruct((1,), f32)),
            in_specs=[pl.BlockSpec(memory_space=pltpu.VMEM)] * 2 + [pl.BlockSpec(memory_space=pltpu.SMEM)],
            out_specs=(pl.BlockSpec(memory_space=pltpu.HBM),) * 2 + (pl.BlockSpec(memory_space=pltpu.SMEM),),
            scratch_shapes=[dma((2, layers))],
            compiler_params=pltpu.CompilerParams(vmem_limit_bytes=1024 * 1024),
            name='router_store',
        )(pltpu.with_memory_space_constraint(d_norm, pltpu.VMEM), pltpu.with_memory_space_constraint(red, pltpu.VMEM), loss)
        return loss.reshape(()), jnp.transpose(red, (0, 2, 1)), d_norm

    tok_spec = P(None, 'dp', None)
    return jax.shard_map(local_step, mesh=mesh, in_specs=(tok_spec, tok_spec, P(None, 'dp', None, None), tok_spec, P()), out_specs=(P(), P(), tok_spec), check_vma=False)
```
